32 devices in a mesh: kring: 8 (over y, x, core), cuts: 4 (over z).
Axes of the slice: x: 2, y: 2, z: 4, core: 2. Of those that a mesh axis runs over, the one named last changes fastest.
Arguments:
- blocks: bfloat16 [8, 768, 4096], P('kring', None, 'cuts'), may hold values from -0.75 to 0.75
- vir_energy: bfloat16 [8, 768], P('kring'), may hold values from 0.29882812 to 3
- occ_energy: bfloat16 [8], P('kring'), may hold values from -1 to -0.19921875
- partner: int32 [1, 8], replicated, may hold values from 0 to 7, each once within a row
Outputs:
- gamma_own: bfloat16 [8, 768, 4096], P('kring', None, 'cuts')
- gamma_partner: bfloat16 [1, 8, 768, 4096], P(None, 'kring', None, 'cuts')
The draws below stay inside these ranges and needn't reach their ends.
Inputs may be any that keep to these rules, and one draw needn't show every extreme that they name: Each row of partner names every k-point exactly once.
All inputs are finite; a program needn't handle non-finite values.
Results may differ from the reference program's by a relative error of at most 0.0055.
Values may be sent and summed in bfloat16 or wider, within the bound.
No kernel may reach another device: no remote copies, remote signals or barrier semaphores. Data moves between devices by JAX's collectives and lax.ppermute only.
A program may use at most 64 MiB of HBM per device.

```python
import jax
import jax.numpy as jnp
from jax import lax

VIRT = 768
NAUX = 4096
NQ = 1
NK = 8


def raised(entries, key, source, target, shards_of, factor):
    def block_of(axis_at):
        return (jnp.arange(entries.shape[axis_at]) // (entries.shape[axis_at] // shards_of)).reshape((-1,) + (1,) * (entries.ndim - 1 - axis_at))

    near = jax.random.permutation(key, shards_of)[block_of(target)]
    second = (block_of(target) + shards_of // 2) % shards_of
    return jnp.where((block_of(source) == near) | (block_of(source) == second), factor * entries, entries)


def shard_levels(key, extent, shards, low, high):
    factor_of = 1.0
    for dim, blocks in shards:
        draws = jax.random.uniform(jax.random.fold_in(jax.random.fold_in(key, 6), dim), (blocks,), jnp.float32, low / len(shards), high / len(shards))
        factor_of = factor_of * jnp.repeat(jnp.exp(draws), extent[dim] // blocks).reshape((-1,) + (1,) * (len(extent) - 1 - dim))
    return factor_of


def noise_with(stream_key, extent, scale, reach, split, heavy, kind=jnp.bfloat16):
    array = scale * jax.random.normal(stream_key, extent, jnp.float32)
    if split:
        array = array * shard_levels(stream_key, extent, split, -0.22, 0.18)
    return jnp.clip(raised(array, jax.random.fold_in(stream_key, 3), *heavy), -reach, reach).astype(kind)


def setup_inputs(seed: int = 0) -> dict:
    key_of = jax.random.split(jax.random.key(seed), 5)
    return {
        "blocks": noise_with(key_of[0], (NK, VIRT, NAUX), (NAUX ** -0.25), 0.75, ((0, 8), (2, 4)), (2, 1, 4, 2.0)),
        "vir_energy": jnp.clip(0.29882812 + 2.7011719 * jax.random.uniform(key_of[1], (NK, VIRT), jnp.float32) ** shard_levels(key_of[1], (NK, VIRT), ((0, 8),), -0.2, 0.2), 0.29882812, 3.0).astype(jnp.bfloat16),
        "occ_energy": jnp.clip(-1.0 + 0.80078125 * jax.random.uniform(key_of[2], (NK,), jnp.float32) ** shard_levels(key_of[2], (NK,), ((0, 8),), -0.2, 0.2), -1.0, -0.19921875).astype(jnp.bfloat16),
        "partner": jax.vmap(lambda own: jax.random.permutation(own, NK))(jax.random.split(key_of[3], NQ)).reshape((NQ, NK)).astype(jnp.int32),
    }


def pair_terms(own_block, mate_block, own_vir, mate_vir, own_occ, mate_occ):
    integral = lax.dot_general(own_block, mate_block, (((1,), (1,)), ((), ())), preferred_element_type=jnp.float32)
    denominator = (own_vir.astype(jnp.float32)[:, None] + mate_vir.astype(jnp.float32)[None, :]) - (own_occ.astype(jnp.float32) + mate_occ.astype(jnp.float32))
    direct = (integral / denominator).astype(jnp.bfloat16)
    paired = (2.0 * direct.astype(jnp.float32) - direct.T.astype(jnp.float32)).astype(jnp.bfloat16)
    own_term = jnp.dot(paired, mate_block, preferred_element_type=jnp.float32)
    partner_term = lax.dot_general(paired, own_block, (((0,), (0,)), ((), ())), preferred_element_type=jnp.float32)
    return own_term, partner_term.astype(jnp.bfloat16)


def reference(blocks, vir_energy, occ_energy, partner):
    def per_kpoint(kpoint):
        own_block = lax.dynamic_index_in_dim(blocks, kpoint, 0, keepdims=False)
        own_vir = lax.dynamic_index_in_dim(vir_energy, kpoint, 0, keepdims=False)
        own_occ = lax.dynamic_index_in_dim(occ_energy, kpoint, 0, keepdims=False)
        own_sum = jnp.zeros((VIRT, NAUX), jnp.float32)
        partner_terms = []
        for transfer in range(NQ):
            mate = lax.dynamic_index_in_dim(partner[transfer], kpoint, 0, keepdims=False).astype(jnp.int32)
            mate_block = lax.dynamic_index_in_dim(blocks, mate, 0, keepdims=False)
            mate_vir = lax.dynamic_index_in_dim(vir_energy, mate, 0, keepdims=False)
            mate_occ = lax.dynamic_index_in_dim(occ_energy, mate, 0, keepdims=False)
            own_term, partner_term = pair_terms(own_block, mate_block, own_vir, mate_vir, own_occ, mate_occ)
            own_sum = own_sum + own_term
            partner_terms.append(partner_term)
        return own_sum.astype(jnp.bfloat16), jnp.stack(partner_terms)

    gamma_own, stacked = lax.map(per_kpoint, jnp.arange(NK, dtype=jnp.int32))
    return gamma_own, jnp.transpose(stacked, (1, 0, 2, 3))
```

```python
import functools

import jax
import jax.numpy as jnp
from jax import lax
from jax.experimental import pallas as pl
from jax.experimental.pallas import tpu as pltpu
from jax.sharding import PartitionSpec as P


INFO = 8
F32, BF16 = jnp.float32, jnp.bfloat16
VMEM_SPEC = pl.BlockSpec(memory_space=pltpu.VMEM)
SMEM_SPEC = pl.BlockSpec(memory_space=pltpu.SMEM)
ANY_SPEC = pl.BlockSpec(memory_space=pl.ANY)


def swap(x, axis, size, flip):
    return lax.ppermute(x, axis, [(i, i ^ flip) for i in range(size)])


def block_order(size):
    bits = size.bit_length() - 1
    return [int(format(i, f"0{bits}b")[::-1], 2) if bits else 0 for i in range(size)]


def choose_kernel(chips, ids_ref, partner_ref, *refs):
    held, outs, sems = refs[: 2 * chips], refs[2 * chips : 3 * chips], refs[-1]
    me = ids_ref[0]
    for hop in range(chips):
        wanted = partner_ref[0, me ^ (2 * hop)] ^ me
        for at in range(2 * chips):

            @pl.when(wanted == at)
            def _():
                pltpu.make_async_copy(held[at], outs[hop], sems.at[hop]).start()

    for hop in range(chips):
        pltpu.make_async_copy(held[0], outs[hop], sems.at[hop]).wait()


def choose(ids, partner, held):
    chips = len(held) // 2
    shape = jax.ShapeDtypeStruct(held[0].shape, held[0].dtype)
    return pl.pallas_call(
        functools.partial(choose_kernel, chips),
        out_shape=[shape] * chips,
        in_specs=[SMEM_SPEC, SMEM_SPEC] + [ANY_SPEC] * len(held),
        out_specs=[VMEM_SPEC] * chips,
        scratch_shapes=[pltpu.SemaphoreType.DMA((chips,))],
        cost_estimate=pl.CostEstimate(
            flops=10**6, bytes_accessed=2 * chips * held[0].size * 2, transcendentals=0
        ),
        name="choose",
    )(ids, partner, *held)


def integral_kernel(cuts, count, ids_ref, own_ref, vir_ref, occ_ref, *refs):
    pieces, (send_ref, keep_ref, total) = refs[:count], refs[count:]
    rows = pieces[0].shape[0] - INFO
    wide = -(-rows // 128) * 128
    place = ids_ref[1]
    own_vir = vir_ref[...].astype(F32)
    own_occ = occ_ref[...].astype(F32)
    for number, piece in enumerate(pieces):
        product = lax.dot_general(
            piece[:rows, :], own_ref[...], (((1,), (1,)), ((), ())), preferred_element_type=F32
        )
        info = piece[rows:, :wide].astype(F32).T
        gap = (own_vir + info[:rows, 0:1]) - (own_occ + info[:rows, 1:2])
        total[number * rows : (number + 1) * rows, :] = product / gap
    step = count * rows // cuts
    order = block_order(cuts)
    for slot, flip in enumerate(order):
        block = total[pl.ds(pl.multiple_of((place ^ flip) * step, step), step), :]
        if slot < cuts // 2:
            keep_ref[slot * step : (slot + 1) * step, :] = block
        else:
            low = (slot - cuts // 2) * step
            send_ref[low : low + step, :] = block.astype(BF16)


def integral(ids, own, vir, occ, pieces, cuts):
    count = len(pieces)
    rows = (pieces[0].shape[0] - INFO) * count
    virt = own.shape[0]
    return pl.pallas_call(
        functools.partial(integral_kernel, cuts, count),
        out_shape=[
            jax.ShapeDtypeStruct((rows // 2, virt), BF16),
            jax.ShapeDtypeStruct((rows // 2, virt), F32),
        ],
        in_specs=[SMEM_SPEC] + [VMEM_SPEC] * (3 + count),
        out_specs=[VMEM_SPEC] * 2,
        scratch_shapes=[pltpu.VMEM((rows, virt), F32)],
        cost_estimate=pl.CostEstimate(
            flops=2 * rows * own.size,
            bytes_accessed=2 * (own.size + rows * own.shape[1]),
            transcendentals=0,
        ),
        name="integral",
    )(ids, own, vir, occ, *pieces)


def reduce_scatter(send, keep, cuts):
    flip = 1
    while True:
        got = swap(send, "cuts", cuts, flip)
        summed = keep + got.astype(F32)
        flip *= 2
        if flip == cuts:
            return summed.astype(BF16)
        half = summed.shape[0] // 2
        keep, send = summed[:half], summed[half:].astype(BF16)


def all_gather(block, cuts):
    have = {0: block}
    flip = cuts // 2
    while flip:
        have.update({at ^ flip: swap(part, "cuts", cuts, flip) for at, part in list(have.items())})
        flip //= 2
    return [have[at] for at in range(cuts)]


def final_kernel(cuts, groups, ids_ref, partner_ref, own_ref, *refs):
    chips = sum(groups)
    parts = refs[: cuts * len(groups)]
    pieces = refs[cuts * len(groups) : cuts * len(groups) + chips]
    gamma_own, gamma_partner, flat, turned, mate, left, right, stage, sems = refs[-9:]
    rows = pieces[0].shape[0] - INFO
    virt = own_ref.shape[0]
    me, place = ids_ref[0], ids_ref[1]
    shift = (partner_ref[0, me] ^ me) // 2
    for hop in range(chips):
        start = pl.multiple_of((shift ^ hop) * rows, rows)
        mate[pl.ds(start, rows), :] = pieces[hop][:rows, :]
    first = 0
    for group, size in enumerate(groups):
        step = size * rows // cuts
        for flip in range(cuts):
            at = (place ^ flip) * step
            hop = first + at // rows
            start = pl.multiple_of((shift ^ hop) * rows + at % rows, step)
            flat[pl.ds(start, step), :] = parts[group * cuts + flip][...].astype(F32)
        first += size
    turned[...] = flat[...].T
    left[...] = (2.0 * turned[...] - flat[...]).astype(BF16)
    right[...] = (2.0 * flat[...] - turned[...]).astype(BF16)
    tile = virt // 3 if virt % 3 == 0 else virt
    copies = []
    for number, (lhs, rhs, out) in enumerate(((left, mate, gamma_own), (right, own_ref, gamma_partner))):
        for low in range(0, virt, tile):
            slot = len(copies)
            stage[slot] = jnp.dot(
                lhs[low : low + tile, :], rhs[...], preferred_element_type=F32
            ).astype(BF16)
            copy = pltpu.make_async_copy(stage.at[slot], out.at[low : low + tile, :], sems.at[slot])
            copy.start()
            copies.append(copy)
    for copy in copies:
        copy.wait()


def final(ids, partner, own, parts, pieces, groups, cuts):
    virt, width = own.shape
    tile = virt // 3 if virt % 3 == 0 else virt
    tiles = 2 * (virt // tile)
    return pl.pallas_call(
        functools.partial(final_kernel, cuts, groups),
        out_shape=[jax.ShapeDtypeStruct((virt, width), BF16)] * 2,
        in_specs=[SMEM_SPEC] * 2 + [VMEM_SPEC] * (1 + len(parts) + len(pieces)),
        out_specs=[ANY_SPEC] * 2,
        scratch_shapes=[
            pltpu.VMEM((virt, virt), F32),
            pltpu.VMEM((virt, virt), F32),
            pltpu.VMEM((virt, width), BF16),
            pltpu.VMEM((virt, virt), BF16),
            pltpu.VMEM((virt, virt), BF16),
            pltpu.VMEM((tiles, tile, width), BF16),
            pltpu.SemaphoreType.DMA((tiles,)),
        ],
        cost_estimate=pl.CostEstimate(
            flops=4 * virt * virt * width, bytes_accessed=8 * virt * width, transcendentals=0
        ),
        name="final",
    )(ids, partner, own, *parts, *pieces)


def on_device(kring, cuts, blocks, vir_energy, occ_energy, partner):
    own = blocks[0]
    virt, width = own.shape
    chips = kring // 2
    rows = virt // chips
    ids = jnp.stack([lax.axis_index("kring"), lax.axis_index("cuts")]).astype(jnp.int32)

    vir_rows = jnp.pad(vir_energy[0].reshape(chips, 1, rows), ((0, 0), (0, 0), (0, width - rows)))
    info = jnp.concatenate(
        [
            vir_rows,
            jnp.broadcast_to(occ_energy.reshape(1, 1, 1), (chips, 1, width)),
            jnp.zeros((chips, INFO - 2, width), BF16),
        ],
        axis=1,
    )
    held = []
    for hop in range(chips):
        piece = jnp.concatenate([own[hop * rows : (hop + 1) * rows], info[hop]])
        if hop:
            piece = swap(piece, "kring", kring, 2 * hop)
        held += [piece, swap(piece, "kring", kring, 1)]

    chosen = choose(ids, partner, held)
    pieces = [chosen[0]] + [swap(chosen[hop], "kring", kring, 2 * hop) for hop in range(1, chips)]

    whole = rows % (8 * cuts) == 0
    groups = [1] * chips if whole else [chips]
    parts, first = [], 0
    for size in groups:
        send, keep = integral(
            ids, own, vir_energy, occ_energy.reshape(1, 1), pieces[first : first + size], cuts
        )
        parts += all_gather(reduce_scatter(send, keep, cuts), cuts)
        first += size
    gamma_own, gamma_partner = final(ids, partner, own, parts, pieces, groups, cuts)
    return gamma_own[None], gamma_partner[None, None]


def solution(mesh):
    kring, cuts = mesh.shape["kring"], mesh.shape["cuts"]
    return jax.shard_map(
        functools.partial(on_device, kring, cuts),
        mesh=mesh,
        in_specs=(P("kring", None, "cuts"), P("kring", None), P("kring"), P()),
        out_specs=(P("kring", None, "cuts"), P(None, "kring", None, "cuts")),
        check_vma=False,
    )
```

```python
import functools

import jax
import jax.numpy as jnp
from jax import lax
from jax.experimental import pallas as pl
from jax.experimental.pallas import tpu as pltpu
from jax.sharding import PartitionSpec as P


INFO = 8
F32, BF16 = jnp.float32, jnp.bfloat16
VMEM_SPEC = pl.BlockSpec(memory_space=pltpu.VMEM)
SMEM_SPEC = pl.BlockSpec(memory_space=pltpu.SMEM)
ANY_SPEC = pl.BlockSpec(memory_space=pl.ANY)


def swap(x, axis, size, flip):
    return lax.ppermute(x, axis, [(i, i ^ flip) for i in range(size)])


def block_order(size):
    bits = size.bit_length() - 1
    return [int(format(i, f"0{bits}b")[::-1], 2) if bits else 0 for i in range(size)]


def choose_kernel(chips, ids_ref, partner_ref, *refs):
    held, outs, sems = refs[: 2 * chips], refs[2 * chips : 3 * chips], refs[-1]
    me = ids_ref[0]
    for hop in range(chips):
        wanted = partner_ref[0, me ^ (2 * hop)] ^ me
        for at in range(2 * chips):

            @pl.when(wanted == at)
            def _():
                pltpu.make_async_copy(held[at], outs[hop], sems.at[hop]).start()

    for hop in range(chips):
        pltpu.make_async_copy(held[0], outs[hop], sems.at[hop]).wait()


def choose(ids, partner, held):
    chips = len(held) // 2
    shape = jax.ShapeDtypeStruct(held[0].shape, held[0].dtype)
    return pl.pallas_call(
        functools.partial(choose_kernel, chips),
        out_shape=[shape] * chips,
        in_specs=[SMEM_SPEC, SMEM_SPEC] + [ANY_SPEC] * len(held),
        out_specs=[VMEM_SPEC] * chips,
        scratch_shapes=[pltpu.SemaphoreType.DMA((chips,))],
        cost_estimate=pl.CostEstimate(
            flops=10**6, bytes_accessed=2 * chips * held[0].size * 2, transcendentals=0
        ),
        name="choose",
        compiler_params=pltpu.CompilerParams(vmem_limit_bytes=6 * 2**20),
    )(ids, partner, *held)


def integral_kernel(cuts, count, ids_ref, own_ref, vir_ref, occ_ref, *refs):
    pieces, (send_ref, keep_ref, total) = refs[:count], refs[count:]
    rows = pieces[0].shape[0] - INFO
    wide = -(-rows // 128) * 128
    place = ids_ref[1]
    own_vir = vir_ref[...].astype(F32)
    own_occ = occ_ref[...].astype(F32)
    for number, piece in enumerate(pieces):
        product = lax.dot_general(
            piece[:rows, :], own_ref[...], (((1,), (1,)), ((), ())), preferred_element_type=F32
        )
        info = piece[rows:, :wide].astype(F32).T
        gap = (own_vir + info[:rows, 0:1]) - (own_occ + info[:rows, 1:2])
        total[number * rows : (number + 1) * rows, :] = product / gap
    step = count * rows // cuts
    order = block_order(cuts)
    for slot, flip in enumerate(order):
        block = total[pl.ds(pl.multiple_of((place ^ flip) * step, step), step), :]
        if slot < cuts // 2:
            keep_ref[slot * step : (slot + 1) * step, :] = block
        else:
            low = (slot - cuts // 2) * step
            send_ref[low : low + step, :] = block.astype(BF16)


def integral(ids, own, vir, occ, pieces, cuts):
    count = len(pieces)
    rows = (pieces[0].shape[0] - INFO) * count
    virt = own.shape[0]
    return pl.pallas_call(
        functools.partial(integral_kernel, cuts, count),
        out_shape=[
            jax.ShapeDtypeStruct((rows // 2, virt), BF16),
            jax.ShapeDtypeStruct((rows // 2, virt), F32),
        ],
        in_specs=[SMEM_SPEC] + [VMEM_SPEC] * (3 + count),
        out_specs=[VMEM_SPEC] * 2,
        scratch_shapes=[pltpu.VMEM((rows, virt), F32)],
        cost_estimate=pl.CostEstimate(
            flops=2 * rows * own.size,
            bytes_accessed=2 * (own.size + rows * own.shape[1]),
            transcendentals=0,
        ),
        name="integral",
        compiler_params=pltpu.CompilerParams(vmem_limit_bytes=10 * 2**20),
    )(ids, own, vir, occ, *pieces)


def reduce_scatter(send, keep, cuts):
    flip = 1
    while True:
        got = swap(send, "cuts", cuts, flip)
        summed = keep + got.astype(F32)
        flip *= 2
        if flip == cuts:
            return summed.astype(BF16)
        half = summed.shape[0] // 2
        keep, send = summed[:half], summed[half:].astype(BF16)


def all_gather(block, cuts):
    have = {0: block}
    flip = cuts // 2
    while flip:
        have.update({at ^ flip: swap(part, "cuts", cuts, flip) for at, part in list(have.items())})
        flip //= 2
    return [have[at] for at in range(cuts)]


def final_kernel(cuts, groups, ids_ref, partner_ref, own_ref, *refs):
    chips = sum(groups)
    parts = refs[: cuts * len(groups)]
    pieces = refs[cuts * len(groups) : cuts * len(groups) + chips]
    gamma_own, gamma_partner, flat, turned, mate, left, right, stage, sems = refs[-9:]
    rows = pieces[0].shape[0] - INFO
    virt = own_ref.shape[0]
    me, place = ids_ref[0], ids_ref[1]
    shift = (partner_ref[0, me] ^ me) // 2
    for hop in range(chips):
        start = pl.multiple_of((shift ^ hop) * rows, rows)
        mate[pl.ds(start, rows), :] = pieces[hop][:rows, :]
    first = 0
    for group, size in enumerate(groups):
        step = size * rows // cuts
        for flip in range(cuts):
            at = (place ^ flip) * step
            hop = first + at // rows
            start = pl.multiple_of((shift ^ hop) * rows + at % rows, step)
            flat[pl.ds(start, step), :] = parts[group * cuts + flip][...].astype(F32)
        first += size
    turned[...] = flat[...].T
    left[...] = (2.0 * turned[...] - flat[...]).astype(BF16)
    right[...] = (2.0 * flat[...] - turned[...]).astype(BF16)
    tile = virt // 3 if virt % 3 == 0 else virt
    copies = []
    for number, (lhs, rhs, out) in enumerate(((left, mate, gamma_own), (right, own_ref, gamma_partner))):
        for low in range(0, virt, tile):
            slot = len(copies)
            stage[slot] = jnp.dot(
                lhs[low : low + tile, :], rhs[...], preferred_element_type=F32
            ).astype(BF16)
            copy = pltpu.make_async_copy(stage.at[slot], out.at[low : low + tile, :], sems.at[slot])
            copy.start()
            copies.append(copy)
    for copy in copies:
        copy.wait()


def final(ids, partner, own, parts, pieces, groups, cuts):
    virt, width = own.shape
    tile = virt // 3 if virt % 3 == 0 else virt
    tiles = 2 * (virt // tile)
    return pl.pallas_call(
        functools.partial(final_kernel, cuts, groups),
        out_shape=[jax.ShapeDtypeStruct((virt, width), BF16)] * 2,
        in_specs=[SMEM_SPEC] * 2 + [VMEM_SPEC] * (1 + len(parts) + len(pieces)),
        out_specs=[ANY_SPEC] * 2,
        scratch_shapes=[
            pltpu.VMEM((virt, virt), F32),
            pltpu.VMEM((virt, virt), F32),
            pltpu.VMEM((virt, width), BF16),
            pltpu.VMEM((virt, virt), BF16),
            pltpu.VMEM((virt, virt), BF16),
            pltpu.VMEM((tiles, tile, width), BF16),
            pltpu.SemaphoreType.DMA((tiles,)),
        ],
        cost_estimate=pl.CostEstimate(
            flops=4 * virt * virt * width, bytes_accessed=8 * virt * width, transcendentals=0
        ),
        name="final",
        compiler_params=pltpu.CompilerParams(vmem_limit_bytes=24 * 2**20),
    )(ids, partner, own, *parts, *pieces)


def on_device(kring, cuts, blocks, vir_energy, occ_energy, partner):
    own = blocks[0]
    virt, width = own.shape
    chips = kring // 2
    rows = virt // chips
    ids = jnp.stack([lax.axis_index("kring"), lax.axis_index("cuts")]).astype(jnp.int32)

    vir_rows = jnp.pad(vir_energy[0].reshape(chips, 1, rows), ((0, 0), (0, 0), (0, width - rows)))
    info = jnp.concatenate(
        [
            vir_rows,
            jnp.broadcast_to(occ_energy.reshape(1, 1, 1), (chips, 1, width)),
            jnp.zeros((chips, INFO - 2, width), BF16),
        ],
        axis=1,
    )
    held = []
    for hop in range(chips):
        piece = jnp.concatenate([own[hop * rows : (hop + 1) * rows], info[hop]])
        if hop:
            piece = swap(piece, "kring", kring, 2 * hop)
        held += [piece, swap(piece, "kring", kring, 1)]

    chosen = choose(ids, partner, held)
    pieces = [chosen[0]] + [swap(chosen[hop], "kring", kring, 2 * hop) for hop in range(1, chips)]

    whole = rows % (8 * cuts) == 0
    groups = [1] * chips if whole else [chips]
    parts, first = [], 0
    for size in groups:
        send, keep = integral(
            ids, own, vir_energy, occ_energy.reshape(1, 1), pieces[first : first + size], cuts
        )
        parts += all_gather(reduce_scatter(send, keep, cuts), cuts)
        first += size
    gamma_own, gamma_partner = final(ids, partner, own, parts, pieces, groups, cuts)
    return gamma_own[None], gamma_partner[None, None]


def solution(mesh):
    kring, cuts = mesh.shape["kring"], mesh.shape["cuts"]
    return jax.shard_map(
        functools.partial(on_device, kring, cuts),
        mesh=mesh,
        in_specs=(P("kring", None, "cuts"), P("kring", None), P("kring"), P()),
        out_specs=(P("kring", None, "cuts"), P(None, "kring", None, "cuts")),
        check_vma=False,
    )
```
